8 devices in a mesh: batch: 2 (over z, y), row: 4 (over x, core).
Axes of the slice: x: 2, y: 2, z: 1, core: 2. Of those that a mesh axis runs over, the one named last changes fastest.
Arguments:
- trans_mat: bfloat16 [16384, 8192], P(('batch', 'row')), parts along dimension 0
- teleport: float32 [16384, 64], P(('batch', 'row')), parts along dimension 0
- dangling: int32 [16384], P(('batch', 'row')), parts along dimension 0
- damping: float32 [16], replicated
- rank_init: float32 [16384, 64], P(('batch', 'row')), parts along dimension 0
Outputs:
- output: float32 [16384, 64], P(('batch', 'row')), parts along dimension 0
There are 2 independent parts. The reference program is written for one: setup_inputs(seed, part) draws one part's arguments, and reference() takes and returns one part's arrays. A program takes and returns all parts, laid end to end along the dimension named above; an argument that names none is the same for every part.
All inputs are finite; a program needn't handle non-finite values.
Results may differ from the reference program's by a relative error of at most 0.001.
Values are sent between devices in bfloat16 or wider.
A program may use at most 1 GiB of HBM per device.

```python
import jax
import jax.numpy as jnp
from jax import lax

NODES = 8192
SEEDS = 64
SWEEPS = 16


def setup_inputs(seed: int = 0, part: int = 0) -> dict:
    base_key = jax.random.key(seed)
    part_key = jax.random.fold_in(base_key, part)
    key_list = jax.random.split(part_key, 8)
    dangling = (jax.random.randint(key_list[0], (NODES,), 0, 100) < 20).astype(jnp.int32)
    popular = jnp.exp(0.8 * jax.random.normal(key_list[1], (NODES,), jnp.float32))
    weights = popular[:, None] * jnp.maximum(jax.random.uniform(key_list[2], (NODES, NODES), jnp.float32) - 0.5, 0.0)
    keep_cols = 1.0 - dangling.astype(jnp.float32)
    col_sum = jnp.sum(weights, axis=0)
    trans_mat = (weights * (keep_cols / jnp.maximum(col_sum, 1e-6))[None, :]).astype(jnp.bfloat16)
    tele_raw = jnp.exp(1.2 * jax.random.normal(key_list[3], (NODES, SEEDS), jnp.float32))
    teleport = tele_raw / jnp.mean(tele_raw, axis=0, keepdims=True)
    col_scale = jax.random.uniform(key_list[4], (1, SEEDS), jnp.float32, 0.3, 3.0)
    rank_init = col_scale * jax.random.uniform(key_list[5], (NODES, SEEDS), jnp.float32, 0.2, 1.8)
    damping = jax.random.uniform(jax.random.key(seed + 1), (SWEEPS,), jnp.float32, 0.75, 0.95)
    return {"trans_mat": trans_mat, "teleport": teleport, "dangling": dangling, "damping": damping, "rank_init": rank_init}


def reference(trans_mat, teleport, dangling, damping, rank_init):
    dang_float = dangling.astype(jnp.float32)

    def one_sweep(rank_cur, factor):
        prod_rows = jnp.dot(trans_mat, rank_cur.astype(jnp.bfloat16), preferred_element_type=jnp.float32)
        dang_mass = jnp.dot(dang_float, rank_cur, preferred_element_type=jnp.float32)
        rank_next = factor * prod_rows + (1.0 - factor) * teleport + (factor / NODES) * dang_mass[None, :]
        return rank_next, None

    rank_final, unused = lax.scan(one_sweep, rank_init, damping)
    return rank_final
```

```python
import functools

import jax
import jax.numpy as jnp
from jax import lax
from jax.experimental import pallas as pl
from jax.experimental.pallas import tpu as pltpu
from jax.sharding import PartitionSpec as P

MESH = pl.DeviceIdType.MESH
TILE = 256
WIDE = 512
RING = 12
OWN, SIB, CROSS, DIAG = range(4)


def _kernel(sweeps, seeds, nodes, mat_hbm, tele_hbm, dang_ref, damp_ref, init_hbm, out_ref,
            mat_t, stage, ranks, tele_t, init_t, local_sum, mass,
            stage_sem, raw_sem, send_sem, recv_sem, fwd_sem, msend_sem, mrecv_sem):
    part_rows = seeds // 2
    wides = nodes // WIDE
    tiles = nodes // TILE
    batch = lax.axis_index("batch")
    row = lax.axis_index("row")
    chip, core = row // 2, row % 2
    sib, cross, diag = chip * 2 + 1 - core, (1 - chip) * 2 + core, (1 - chip) * 2 + 1 - core
    blocks = (row, sib, cross, diag)

    def own_copy(par, ph, target):
        return pltpu.make_async_remote_copy(
            src_ref=ranks.at[par, OWN, ph], dst_ref=ranks.at[par, target, ph],
            send_sem=send_sem.at[par, ph, target - 1], recv_sem=recv_sem.at[par, ph, target - 1],
            device_id=(batch, blocks[target]), device_id_type=MESH)

    def fwd_copy(par, ph):
        return pltpu.make_async_remote_copy(
            src_ref=ranks.at[par, CROSS, ph], dst_ref=ranks.at[par, DIAG, ph],
            send_sem=fwd_sem.at[par, ph], recv_sem=recv_sem.at[par, ph, DIAG - 1],
            device_id=(batch, sib), device_id_type=MESH)

    def mass_copy(par, ph, target):
        return pltpu.make_async_remote_copy(
            src_ref=mass.at[par, ph, OWN], dst_ref=mass.at[par, ph, target],
            send_sem=msend_sem.at[par, ph, target - 1], recv_sem=mrecv_sem.at[par, ph, target - 1],
            device_id=(batch, blocks[target]), device_id_type=MESH)

    def send(par, ph):
        own_copy(par, ph, CROSS).start()
        own_copy(par, ph, SIB).start()

    def mass_part(val, n, width):
        part = jnp.zeros((val.shape[0], 128), jnp.float32)
        for i in range(width // 128):
            r = n * (width // 128) + i
            part = part + val[:, i * 128:(i + 1) * 128] * dang_ref[r:r + 1, :].astype(jnp.float32)
        return part

    def send_mass(par, ph, part):
        mass[par, ph, OWN, 0:1, 0:part_rows] = jnp.sum(part.T, axis=0, keepdims=True)
        for target in (CROSS, DIAG, SIB):
            mass_copy(par, ph, target).start()

    def get_mass(par, ph):
        for target in (CROSS, DIAG, SIB):
            mass_copy(par, ph, target).wait_recv()
        line = [mass[par, ph, s, 0:1, 0:part_rows] for s in range(4)]
        total = (line[OWN] + line[SIB]) + (line[CROSS] + line[DIAG])
        return jnp.broadcast_to(total, (128, part_rows)).T

    init_copy = pltpu.make_async_copy(init_hbm, init_t, raw_sem.at[0])
    tele_copy = pltpu.make_async_copy(tele_hbm, tele_t, raw_sem.at[1])
    init_copy.start()

    def stage_copy(s, c, buf):
        return pltpu.make_async_copy(
            mat_hbm.at[pl.ds(pl.multiple_of(c * TILE, TILE), TILE), pl.ds(pl.multiple_of(blocks[s] * nodes, nodes), nodes)],
            stage.at[buf], stage_sem.at[buf])

    for i in range(RING):
        stage_copy(i // tiles, i % tiles, i).start()
    tele_copy.start()

    mass[:, :, OWN] = jnp.zeros_like(mass[:, :, OWN])
    barrier = pltpu.get_barrier_semaphore()
    for peer in (sib, cross, diag):
        pl.semaphore_signal(barrier, inc=1, device_id=(batch, peer), device_id_type=MESH)
    pl.semaphore_wait(barrier, 3)

    init_copy.wait()
    for ph in range(2):
        rows = slice(ph * part_rows, (ph + 1) * part_rows)
        part = jnp.zeros((part_rows, 128), jnp.float32)
        for n in range(wides):
            val = init_t[rows, n * WIDE:(n + 1) * WIDE]
            ranks[0, OWN, ph, :, n * WIDE:(n + 1) * WIDE] = val.astype(jnp.bfloat16)
            part = part + mass_part(val, n, WIDE)
        send(0, ph)
        send_mass(0, ph, part)
    tele_copy.wait()

    total = 4 * tiles

    for s in range(4):
        def load_rows(c, carry, s=s):
            i = s * tiles + c
            buf = lax.rem(i, RING)
            stage_copy(s, c, buf).wait()
            for u in range(2):
                @pl.when(lax.rem(c, 2) == u)
                def _(u=u):
                    for k in range(tiles):
                        mat_t[s, c // 2, k * TILE:(k + 1) * TILE, u * TILE:(u + 1) * TILE] = stage[buf, :, k * TILE:(k + 1) * TILE].T
            for s2 in range(s, 4):
                @pl.when(jnp.logical_and(i + RING >= s2 * tiles, i + RING < (s2 + 1) * tiles))
                def _(s2=s2):
                    stage_copy(s2, i + RING - s2 * tiles, buf).start()
            return carry

        lax.fori_loop(0, tiles, load_rows, 0)

    def lhs(par, s, ph):
        val = ranks[par, s, ph]
        return jnp.concatenate([val] * 4, axis=0)

    def dot(left, s, n):
        return jnp.dot(left, mat_t[s, n], preferred_element_type=jnp.float32)

    def local_pass(par):
        left = jnp.concatenate([ranks[par, OWN, 0], ranks[par, OWN, 1]] * 2, axis=0)
        for n in range(wides):
            local_sum[:, n * WIDE:(n + 1) * WIDE] = dot(left, OWN, n)[:seeds]
        for ph in range(2):
            own_copy(par, ph, SIB).wait_recv()
        left = jnp.concatenate([ranks[par, SIB, 0], ranks[par, SIB, 1]] * 2, axis=0)
        for n in range(wides):
            cols = slice(n * WIDE, (n + 1) * WIDE)
            local_sum[:, cols] = local_sum[:, cols] + dot(left, SIB, n)[:seeds]

    def remote_pass(par, ph, t, store):
        rows = slice(ph * part_rows, (ph + 1) * part_rows)
        own_copy(par, ph, CROSS).wait_recv()
        fwd_copy(par, ph).start()
        left = lhs(par, CROSS, ph)
        for n in range(wides):
            cols = slice(n * WIDE, (n + 1) * WIDE)
            local_sum[rows, cols] = local_sum[rows, cols] + dot(left, CROSS, n)[:part_rows]
        fwd_copy(par, ph).wait_recv()
        msum = get_mass(par, ph)
        factor = damp_ref[t]
        add = (factor * (1.0 / (4 * nodes))) * msum
        add = jnp.concatenate([add] * (WIDE // 128), axis=1)
        left = lhs(par, DIAG, ph)
        for n in range(wides):
            cols = slice(n * WIDE, (n + 1) * WIDE)
            total = local_sum[rows, cols] + dot(left, DIAG, n)[:part_rows]
            store(n, factor * total + (1.0 - factor) * tele_t[rows, cols] + add)

    def done(par, ph):
        own_copy(par, ph, SIB).wait_send()
        own_copy(par, ph, CROSS).wait_send()
        fwd_copy(par, ph).wait_send()
        for target in (CROSS, DIAG, SIB):
            mass_copy(par, ph, target).wait_send()

    def sweep(t, carry):
        par = lax.rem(t, 2)
        nxt = 1 - par
        local_pass(par)
        for ph in range(2):
            parts = []

            def store(n, val, ph=ph, parts=parts):
                ranks[nxt, OWN, ph, :, n * WIDE:(n + 1) * WIDE] = val.astype(jnp.bfloat16)
                parts.append(mass_part(val, n, WIDE))

            remote_pass(par, ph, t, store)
            done(par, ph)
            send(nxt, ph)
            send_mass(nxt, ph, functools.reduce(jnp.add, parts))
        return carry

    lax.fori_loop(0, sweeps - 1, sweep, 0)
    last = sweeps - 1
    par = last % 2
    local_pass(par)
    for ph in range(2):
        def store(n, val, ph=ph):
            out_ref[ph * part_rows:(ph + 1) * part_rows, n * WIDE:(n + 1) * WIDE] = val

        remote_pass(par, ph, last, store)
        done(par, ph)


def solution(mesh):
    spec_rows = P(("batch", "row"), None)
    spec_vec = P(("batch", "row"))

    def local_sweeps(mat_rows, tele_rows, dang_rows, damping, start_rows):
        nodes, seeds = start_rows.shape
        sweeps = damping.shape[0]
        hbm = pl.BlockSpec(memory_space=pl.ANY)
        vmem = pl.BlockSpec(memory_space=pltpu.VMEM)
        dma = pltpu.SemaphoreType.DMA
        out = pl.pallas_call(
            functools.partial(_kernel, sweeps, seeds, nodes),
            out_shape=jax.ShapeDtypeStruct((seeds, nodes), jnp.float32),
            in_specs=[hbm, hbm, vmem, pl.BlockSpec(memory_space=pltpu.SMEM), hbm],
            out_specs=vmem,
            scratch_shapes=[
                pltpu.VMEM((4, nodes // WIDE, nodes, WIDE), jnp.bfloat16),
                pltpu.VMEM((RING, TILE, nodes), jnp.bfloat16),
                pltpu.VMEM((2, 4, 2, seeds // 2, nodes), jnp.bfloat16),
                pltpu.VMEM((seeds, nodes), jnp.float32),
                pltpu.VMEM((seeds, nodes), jnp.float32),
                pltpu.VMEM((seeds, nodes), jnp.float32),
                pltpu.VMEM((2, 2, 4, 8, 128), jnp.float32),
                dma((RING,)), dma((2,)), dma((2, 2, 2)), dma((2, 2, 3)), dma((2, 2)), dma((2, 2, 3)), dma((2, 2, 3)),
            ],
            compiler_params=pltpu.CompilerParams(collective_id=0, has_side_effects=True, vmem_limit_bytes=63 * 2**20),
        )(mat_rows, tele_rows.T, dang_rows.reshape(-1, 128), damping, start_rows.T)
        return out.T

    return jax.shard_map(local_sweeps, mesh=mesh, in_specs=(spec_rows, spec_rows, spec_vec, P(None), spec_rows), out_specs=spec_rows, check_vma=False)
```

```python
import functools

import jax
import jax.numpy as jnp
from jax import lax
from jax.experimental import pallas as pl
from jax.experimental.pallas import tpu as pltpu
from jax.sharding import PartitionSpec as P

MESH = pl.DeviceIdType.MESH
TILE = 256
WIDE = 512
RING = 6
CROSS_AT = 11
OWN, SIB, CROSS, DIAG = range(4)


def _kernel(sweeps, seeds, nodes, mat_hbm, tele_hbm, dang_ref, damp_ref, init_hbm, out_ref,
            mat_t, stage, ranks, tele_t, init_t, local_sum, mass,
            stage_sem, raw_sem, send_sem, recv_sem, fwd_sem, msend_sem, mrecv_sem):
    part_rows = seeds // 2
    wides = nodes // WIDE
    tiles = nodes // TILE
    batch = lax.axis_index("batch")
    row = lax.axis_index("row")
    chip, core = row // 2, row % 2
    sib, cross, diag = chip * 2 + 1 - core, (1 - chip) * 2 + core, (1 - chip) * 2 + 1 - core
    blocks = (row, sib, cross, diag)

    def own_copy(par, ph, target):
        return pltpu.make_async_remote_copy(
            src_ref=ranks.at[par, OWN, ph], dst_ref=ranks.at[par, target, ph],
            send_sem=send_sem.at[par, ph, target - 1], recv_sem=recv_sem.at[par, ph, target - 1],
            device_id=(batch, blocks[target]), device_id_type=MESH)

    def fwd_copy(par, ph):
        return pltpu.make_async_remote_copy(
            src_ref=ranks.at[par, CROSS, ph], dst_ref=ranks.at[par, DIAG, ph],
            send_sem=fwd_sem.at[par, ph], recv_sem=recv_sem.at[par, ph, DIAG - 1],
            device_id=(batch, sib), device_id_type=MESH)

    def mass_copy(par, ph, target):
        return pltpu.make_async_remote_copy(
            src_ref=mass.at[par, ph, OWN], dst_ref=mass.at[par, ph, target],
            send_sem=msend_sem.at[par, ph, target - 1], recv_sem=mrecv_sem.at[par, ph, target - 1],
            device_id=(batch, blocks[target]), device_id_type=MESH)

    def send(par, ph):
        own_copy(par, ph, CROSS).start()
        own_copy(par, ph, SIB).start()

    def mass_part(val, n, width):
        part = jnp.zeros((val.shape[0], 128), jnp.float32)
        for i in range(width // 128):
            r = n * (width // 128) + i
            part = part + val[:, i * 128:(i + 1) * 128] * dang_ref[r:r + 1, :].astype(jnp.float32)
        return part

    def send_mass(par, ph, part):
        mass[par, ph, OWN, 0:1, 0:part_rows] = jnp.sum(part.T, axis=0, keepdims=True)
        for target in (CROSS, DIAG, SIB):
            mass_copy(par, ph, target).start()

    def get_mass(par, ph):
        for target in (CROSS, DIAG, SIB):
            mass_copy(par, ph, target).wait_recv()
        line = [mass[par, ph, s, 0:1, 0:part_rows] for s in range(4)]
        total = (line[OWN] + line[SIB]) + (line[CROSS] + line[DIAG])
        return jnp.broadcast_to(total, (128, part_rows)).T

    init_copy = pltpu.make_async_copy(init_hbm, init_t, raw_sem.at[0])
    tele_copy = pltpu.make_async_copy(tele_hbm, tele_t, raw_sem.at[1])
    init_copy.start()

    def stage_copy(i):
        s, n = i // wides, i % wides
        block = ((chip + s // 2) % 2) * 2 + (core + s % 2) % 2
        return pltpu.make_async_copy(
            mat_hbm.at[pl.ds(pl.multiple_of(n * WIDE, WIDE), WIDE), pl.ds(pl.multiple_of(block * nodes, nodes), nodes)],
            stage.at[i % RING], stage_sem.at[i % RING])

    for i in range(RING):
        stage_copy(i).start()
    tele_copy.start()

    mass[:, :, OWN] = jnp.zeros_like(mass[:, :, OWN])
    barrier = pltpu.get_barrier_semaphore()
    for peer in (sib, cross, diag):
        pl.semaphore_signal(barrier, inc=1, device_id=(batch, peer), device_id_type=MESH)
    pl.semaphore_wait(barrier, 3)

    init_copy.wait()
    for ph in range(2):
        rows = slice(ph * part_rows, (ph + 1) * part_rows)
        part = jnp.zeros((part_rows, 128), jnp.float32)
        for n in range(wides):
            val = init_t[rows, n * WIDE:(n + 1) * WIDE]
            ranks[0, OWN, ph, :, n * WIDE:(n + 1) * WIDE] = val.astype(jnp.bfloat16)
            part = part + mass_part(val, n, WIDE)
        send(0, ph)
        send_mass(0, ph, part)
    tele_copy.wait()

    def cols_of(n):
        return slice(n * WIDE, (n + 1) * WIDE)

    def lhs(par, s, ph):
        val = ranks[par, s, ph]
        return jnp.concatenate([val] * 4, axis=0)

    def dot(left, s, n):
        return jnp.dot(left, mat_t[s, n], preferred_element_type=jnp.float32)

    def local_pass(par):
        left = jnp.concatenate([ranks[par, OWN, 0], ranks[par, OWN, 1]] * 2, axis=0)
        for n in range(wides):
            local_sum[:, n * WIDE:(n + 1) * WIDE] = dot(left, OWN, n)[:seeds]
        for ph in range(2):
            own_copy(par, ph, SIB).wait_recv()
        left = jnp.concatenate([ranks[par, SIB, 0], ranks[par, SIB, 1]] * 2, axis=0)
        for n in range(wides):
            cols = slice(n * WIDE, (n + 1) * WIDE)
            local_sum[:, cols] = local_sum[:, cols] + dot(left, SIB, n)[:seeds]

    def remote_pass(par, ph, t, store):
        rows = slice(ph * part_rows, (ph + 1) * part_rows)
        own_copy(par, ph, CROSS).wait_recv()
        fwd_copy(par, ph).start()
        left = lhs(par, CROSS, ph)
        for n in range(wides):
            cols = slice(n * WIDE, (n + 1) * WIDE)
            local_sum[rows, cols] = local_sum[rows, cols] + dot(left, CROSS, n)[:part_rows]
        fwd_copy(par, ph).wait_recv()
        msum = get_mass(par, ph)
        factor = damp_ref[t]
        add = (factor * (1.0 / (4 * nodes))) * msum
        add = jnp.concatenate([add] * (WIDE // 128), axis=1)
        left = lhs(par, DIAG, ph)
        for n in range(wides):
            cols = slice(n * WIDE, (n + 1) * WIDE)
            total = local_sum[rows, cols] + dot(left, DIAG, n)[:part_rows]
            store(n, factor * total + (1.0 - factor) * tele_t[rows, cols] + add)

    def done(par, ph):
        own_copy(par, ph, SIB).wait_send()
        own_copy(par, ph, CROSS).wait_send()
        fwd_copy(par, ph).wait_send()
        for target in (CROSS, DIAG, SIB):
            mass_copy(par, ph, target).wait_send()

    def load_piece(i):
        stage_copy(i).wait()
        for k in range(tiles):
            for u in range(WIDE // TILE):
                mat_t[i // wides, i % wides, k * TILE:(k + 1) * TILE, u * TILE:(u + 1) * TILE] = (
                    stage[i % RING, u * TILE:(u + 1) * TILE, k * TILE:(k + 1) * TILE].T)

        if i + RING < 4 * wides:
            stage_copy(i + RING).start()

    def both(par, s):
        return jnp.concatenate([ranks[par, s, 0], ranks[par, s, 1]] * 2, axis=0)

    def first_dot(s, n):
        prod = dot(both(0, s), s, n)[:seeds]
        local_sum[:, cols_of(n)] = prod if s == OWN else local_sum[:, cols_of(n)] + prod

    for i in range(4 * wides):
        if i == wides + 1:
            for ph in range(2):
                own_copy(0, ph, SIB).wait_recv()
        if i == CROSS_AT:
            for ph in range(2):
                own_copy(0, ph, CROSS).wait_recv()
                fwd_copy(0, ph).start()
        load_piece(i)
        if 1 <= i <= 2 * wides:
            first_dot((i - 1) // wides, (i - 1) % wides)
        if i >= 3 * wides:
            first_dot(CROSS, i - 3 * wides)
    first_parts = []
    for ph in range(2):
        fwd_copy(0, ph).wait_recv()
    sums = [get_mass(0, ph) for ph in range(2)]
    add = (damp_ref[0] * (1.0 / (4 * nodes))) * jnp.concatenate(sums, axis=0)
    add = jnp.concatenate([add] * (WIDE // 128), axis=1)
    for n in range(wides):
        total = local_sum[:, cols_of(n)] + dot(both(0, DIAG), DIAG, n)[:seeds]
        val = damp_ref[0] * total + (1.0 - damp_ref[0]) * tele_t[:, cols_of(n)] + add
        for ph in range(2):
            ranks[1, OWN, ph, :, cols_of(n)] = val[ph * part_rows:(ph + 1) * part_rows].astype(jnp.bfloat16)
        first_parts.append(mass_part(val, n, WIDE))
    first_part = functools.reduce(jnp.add, first_parts)
    for ph in range(2):
        done(0, ph)
    for ph in range(2):
        send(1, ph)
        send_mass(1, ph, first_part[ph * part_rows:(ph + 1) * part_rows])

    def sweep(t, carry):
        par = lax.rem(t, 2)
        nxt = 1 - par
        local_pass(par)
        for ph in range(2):
            parts = []

            def store(n, val, ph=ph, parts=parts):
                ranks[nxt, OWN, ph, :, n * WIDE:(n + 1) * WIDE] = val.astype(jnp.bfloat16)
                parts.append(mass_part(val, n, WIDE))

            remote_pass(par, ph, t, store)
            done(par, ph)
            send(nxt, ph)
            send_mass(nxt, ph, functools.reduce(jnp.add, parts))
        return carry

    lax.fori_loop(1, sweeps - 1, sweep, 0)
    last = sweeps - 1
    par = last % 2
    local_pass(par)
    for ph in range(2):
        def store(n, val, ph=ph):
            out_ref[ph * part_rows:(ph + 1) * part_rows, n * WIDE:(n + 1) * WIDE] = val

        remote_pass(par, ph, last, store)
        done(par, ph)


def solution(mesh):
    spec_rows = P(("batch", "row"), None)
    spec_vec = P(("batch", "row"))

    def local_sweeps(mat_rows, tele_rows, dang_rows, damping, start_rows):
        nodes, seeds = start_rows.shape
        sweeps = damping.shape[0]
        hbm = pl.BlockSpec(memory_space=pl.ANY)
        vmem = pl.BlockSpec(memory_space=pltpu.VMEM)
        dma = pltpu.SemaphoreType.DMA
        out = pl.pallas_call(
            functools.partial(_kernel, sweeps, seeds, nodes),
            out_shape=jax.ShapeDtypeStruct((seeds, nodes), jnp.float32),
            in_specs=[hbm, hbm, vmem, pl.BlockSpec(memory_space=pltpu.SMEM), hbm],
            out_specs=vmem,
            scratch_shapes=[
                pltpu.VMEM((4, nodes // WIDE, nodes, WIDE), jnp.bfloat16),
                pltpu.VMEM((RING, WIDE, nodes), jnp.bfloat16),
                pltpu.VMEM((2, 4, 2, seeds // 2, nodes), jnp.bfloat16),
                pltpu.VMEM((seeds, nodes), jnp.float32),
                pltpu.VMEM((seeds, nodes), jnp.float32),
                pltpu.VMEM((seeds, nodes), jnp.float32),
                pltpu.VMEM((2, 2, 4, 8, 128), jnp.float32),
                dma((RING,)), dma((2,)), dma((2, 2, 2)), dma((2, 2, 3)), dma((2, 2)), dma((2, 2, 3)), dma((2, 2, 3)),
            ],
            compiler_params=pltpu.CompilerParams(collective_id=0, has_side_effects=True, vmem_limit_bytes=63 * 2**20),
        )(mat_rows, tele_rows.T, dang_rows.reshape(-1, 128), damping, start_rows.T)
        return out.T

    return jax.shard_map(local_sweeps, mesh=mesh, in_specs=(spec_rows, spec_rows, spec_vec, P(None), spec_rows), out_specs=spec_rows, check_vma=False)
```

```python
import functools

import jax
import jax.numpy as jnp
from jax import lax
from jax.experimental import pallas as pl
from jax.experimental.pallas import tpu as pltpu
from jax.sharding import PartitionSpec as P

MESH = pl.DeviceIdType.MESH
TILE = 256
WIDE = 512
RING = 6
CROSS_AT = 11
LATER = {12: ((2, 0), (2, 1)), 13: ((2, 2), (2, 3)), 14: ((3, 0), (3, 1)), 15: ((3, 2),)}
OWN, SIB, CROSS, DIAG = range(4)


def _kernel(sweeps, seeds, nodes, mat_hbm, tele_hbm, dang_ref, damp_ref, init_hbm, out_ref,
            mat_t, stage, ranks, tele_t, init_t, local_sum, mass,
            stage_sem, raw_sem, send_sem, recv_sem, msend_sem, mrecv_sem):
    part_rows = seeds // 2
    wides = nodes // WIDE
    tiles = nodes // TILE
    batch = lax.axis_index("batch")
    row = lax.axis_index("row")
    chip, core = row // 2, row % 2
    sib, cross, diag = chip * 2 + 1 - core, (1 - chip) * 2 + core, (1 - chip) * 2 + 1 - core
    blocks = (row, sib, cross, diag)

    def own_copy(par, ph, target):
        return pltpu.make_async_remote_copy(
            src_ref=ranks.at[par, OWN, ph], dst_ref=ranks.at[par, target, ph],
            send_sem=send_sem.at[par, ph], recv_sem=recv_sem.at[par, ph, target - 1],
            device_id=(batch, blocks[target]), device_id_type=MESH)

    def fwd_copy(par, ph):
        return pltpu.make_async_remote_copy(
            src_ref=ranks.at[par, CROSS, ph], dst_ref=ranks.at[par, DIAG, ph],
            send_sem=send_sem.at[par, ph], recv_sem=recv_sem.at[par, ph, DIAG - 1],
            device_id=(batch, sib), device_id_type=MESH)

    def mass_copy(par, ph, target):
        return pltpu.make_async_remote_copy(
            src_ref=mass.at[par, ph, OWN], dst_ref=mass.at[par, ph, target],
            send_sem=msend_sem.at[par, ph], recv_sem=mrecv_sem.at[par, ph],
            device_id=(batch, blocks[target]), device_id_type=MESH)

    def mass_all(par, ph):
        return pltpu.make_async_remote_copy(
            src_ref=mass.at[par, ph, 1:4], dst_ref=mass.at[par, ph, 1:4],
            send_sem=msend_sem.at[par, ph], recv_sem=mrecv_sem.at[par, ph],
            device_id=(batch, sib), device_id_type=MESH)

    def send(par, ph):
        own_copy(par, ph, CROSS).start()
        own_copy(par, ph, SIB).start()

    def mass_part(val, n, width):
        part = jnp.zeros((val.shape[0], 128), jnp.float32)
        for i in range(width // 128):
            r = n * (width // 128) + i
            part = part + val[:, i * 128:(i + 1) * 128] * dang_ref[r:r + 1, :].astype(jnp.float32)
        return part

    def send_mass(par, ph, part):
        mass[par, ph, OWN, 0:1, 0:part_rows] = jnp.sum(part.T, axis=0, keepdims=True)
        for target in (CROSS, DIAG, SIB):
            mass_copy(par, ph, target).start()

    def get_mass(par, ph):
        mass_all(par, ph).wait_recv()
        line = [mass[par, ph, s, 0:1, 0:part_rows] for s in range(4)]
        total = (line[OWN] + line[SIB]) + (line[CROSS] + line[DIAG])
        return jnp.broadcast_to(total, (128, part_rows)).T

    init_copy = pltpu.make_async_copy(init_hbm, init_t, raw_sem.at[0])
    tele_copy = pltpu.make_async_copy(tele_hbm, tele_t, raw_sem.at[1])
    init_copy.start()

    def stage_copy(i):
        s, n = i // wides, i % wides
        block = ((chip + s // 2) % 2) * 2 + (core + s % 2) % 2
        return pltpu.make_async_copy(
            mat_hbm.at[pl.ds(pl.multiple_of(n * WIDE, WIDE), WIDE), pl.ds(pl.multiple_of(block * nodes, nodes), nodes)],
            stage.at[i % RING], stage_sem.at[i % RING])

    for i in range(RING):
        stage_copy(i).start()
    tele_copy.start()

    mass[:, :, OWN] = jnp.zeros_like(mass[:, :, OWN])
    barrier = pltpu.get_barrier_semaphore()
    for peer in (sib, cross, diag):
        pl.semaphore_signal(barrier, inc=1, device_id=(batch, peer), device_id_type=MESH)
    pl.semaphore_wait(barrier, 3)

    init_copy.wait()
    for ph in range(2):
        rows = slice(ph * part_rows, (ph + 1) * part_rows)
        part = jnp.zeros((part_rows, 128), jnp.float32)
        for n in range(wides):
            val = init_t[rows, n * WIDE:(n + 1) * WIDE]
            ranks[0, OWN, ph, :, n * WIDE:(n + 1) * WIDE] = val.astype(jnp.bfloat16)
            part = part + mass_part(val, n, WIDE)
        send(0, ph)
        send_mass(0, ph, part)
    tele_copy.wait()

    def cols_of(n):
        return slice(n * WIDE, (n + 1) * WIDE)

    def lhs(par, s, ph):
        val = ranks[par, s, ph]
        return jnp.concatenate([val] * 4, axis=0)

    def dot(left, s, n):
        return jnp.dot(left, mat_t[s, n], preferred_element_type=jnp.float32)

    def local_pass(par):
        left = jnp.concatenate([ranks[par, OWN, 0], ranks[par, OWN, 1]] * 2, axis=0)
        for n in range(wides):
            local_sum[:, n * WIDE:(n + 1) * WIDE] = dot(left, OWN, n)[:seeds]
        for ph in range(2):
            own_copy(par, ph, SIB).wait_recv()
        left = jnp.concatenate([ranks[par, SIB, 0], ranks[par, SIB, 1]] * 2, axis=0)
        for n in range(wides):
            cols = slice(n * WIDE, (n + 1) * WIDE)
            local_sum[:, cols] = local_sum[:, cols] + dot(left, SIB, n)[:seeds]

    def remote_pass(par, ph, t, store):
        rows = slice(ph * part_rows, (ph + 1) * part_rows)
        own_copy(par, ph, CROSS).wait_recv()
        fwd_copy(par, ph).start()
        left = lhs(par, CROSS, ph)
        for n in range(wides):
            cols = slice(n * WIDE, (n + 1) * WIDE)
            local_sum[rows, cols] = local_sum[rows, cols] + dot(left, CROSS, n)[:part_rows]
        fwd_copy(par, ph).wait_recv()
        msum = get_mass(par, ph)
        factor = damp_ref[t]
        add = (factor * (1.0 / (4 * nodes))) * msum
        add = jnp.concatenate([add] * (WIDE // 128), axis=1)
        left = lhs(par, DIAG, ph)
        for n in range(wides):
            cols = slice(n * WIDE, (n + 1) * WIDE)
            total = local_sum[rows, cols] + dot(left, DIAG, n)[:part_rows]
            store(n, factor * total + (1.0 - factor) * tele_t[rows, cols] + add)

    def done(par, ph):
        pltpu.make_async_remote_copy(
            src_ref=ranks.at[par, 0:3, ph], dst_ref=ranks.at[par, 0:3, ph],
            send_sem=send_sem.at[par, ph], recv_sem=recv_sem.at[par, ph, 0],
            device_id=(batch, sib), device_id_type=MESH).wait_send()
        mass_all(par, ph).wait_send()

    def load_piece(i):
        stage_copy(i).wait()
        for k in range(tiles):
            for u in range(WIDE // TILE):
                mat_t[i // wides, i % wides, k * TILE:(k + 1) * TILE, u * TILE:(u + 1) * TILE] = (
                    stage[i % RING, u * TILE:(u + 1) * TILE, k * TILE:(k + 1) * TILE].T)

        if i + RING < 4 * wides:
            stage_copy(i + RING).start()

    def both(par, s):
        return jnp.concatenate([ranks[par, s, 0], ranks[par, s, 1]] * 2, axis=0)

    def first_dot(s, n):
        prod = dot(both(0, s), s, n)[:seeds]
        local_sum[:, cols_of(n)] = prod if s == OWN else local_sum[:, cols_of(n)] + prod

    for i in range(4 * wides):
        if i == wides + 1:
            for ph in range(2):
                own_copy(0, ph, SIB).wait_recv()
        if i == CROSS_AT:
            for ph in range(2):
                own_copy(0, ph, CROSS).wait_recv()
                fwd_copy(0, ph).start()
        load_piece(i)
        if 1 <= i <= 2 * wides:
            first_dot((i - 1) // wides, (i - 1) % wides)
        if i == 4 * wides - 2:
            for ph in range(2):
                fwd_copy(0, ph).wait_recv()
        for s, n in LATER.get(i, ()):
            first_dot(s, n)
    first_parts = []
    sums = [get_mass(0, ph) for ph in range(2)]
    add = (damp_ref[0] * (1.0 / (4 * nodes))) * jnp.concatenate(sums, axis=0)
    add = jnp.concatenate([add] * (WIDE // 128), axis=1)
    for n in range(wides):
        total = local_sum[:, cols_of(n)]
        if n == wides - 1:
            total = total + dot(both(0, DIAG), DIAG, n)[:seeds]
        val = damp_ref[0] * total + (1.0 - damp_ref[0]) * tele_t[:, cols_of(n)] + add
        for ph in range(2):
            ranks[1, OWN, ph, :, cols_of(n)] = val[ph * part_rows:(ph + 1) * part_rows].astype(jnp.bfloat16)
        first_parts.append(mass_part(val, n, WIDE))
    first_part = functools.reduce(jnp.add, first_parts)
    for ph in range(2):
        done(0, ph)
    for ph in range(2):
        send(1, ph)
        send_mass(1, ph, first_part[ph * part_rows:(ph + 1) * part_rows])

    def sweep(t, carry):
        par = lax.rem(t, 2)
        nxt = 1 - par
        local_pass(par)
        for ph in range(2):
            parts = []

            def store(n, val, ph=ph, parts=parts):
                ranks[nxt, OWN, ph, :, n * WIDE:(n + 1) * WIDE] = val.astype(jnp.bfloat16)
                parts.append(mass_part(val, n, WIDE))

            remote_pass(par, ph, t, store)
            done(par, ph)
            send(nxt, ph)
            send_mass(nxt, ph, functools.reduce(jnp.add, parts))
        return carry

    lax.fori_loop(1, sweeps - 1, sweep, 0)
    last = sweeps - 1
    par = last % 2
    local_pass(par)
    for ph in range(2):
        def store(n, val, ph=ph):
            out_ref[ph * part_rows:(ph + 1) * part_rows, n * WIDE:(n + 1) * WIDE] = val

        remote_pass(par, ph, last, store)
        done(par, ph)


def solution(mesh):
    spec_rows = P(("batch", "row"), None)
    spec_vec = P(("batch", "row"))

    def local_sweeps(mat_rows, tele_rows, dang_rows, damping, start_rows):
        nodes, seeds = start_rows.shape
        sweeps = damping.shape[0]
        hbm = pl.BlockSpec(memory_space=pl.ANY)
        vmem = pl.BlockSpec(memory_space=pltpu.VMEM)
        dma = pltpu.SemaphoreType.DMA
        out = pl.pallas_call(
            functools.partial(_kernel, sweeps, seeds, nodes),
            out_shape=jax.ShapeDtypeStruct((seeds, nodes), jnp.float32),
            in_specs=[hbm, hbm, vmem, pl.BlockSpec(memory_space=pltpu.SMEM), hbm],
            out_specs=vmem,
            scratch_shapes=[
                pltpu.VMEM((4, nodes // WIDE, nodes, WIDE), jnp.bfloat16),
                pltpu.VMEM((RING, WIDE, nodes), jnp.bfloat16),
                pltpu.VMEM((2, 4, 2, seeds // 2, nodes), jnp.bfloat16),
                pltpu.VMEM((seeds, nodes), jnp.float32),
                pltpu.VMEM((seeds, nodes), jnp.float32),
                pltpu.VMEM((seeds, nodes), jnp.float32),
                pltpu.VMEM((2, 2, 4, 8, 128), jnp.float32),
                dma((RING,)), dma((2,)), dma((2, 2)), dma((2, 2, 3)), dma((2, 2)), dma((2, 2)),
            ],
            compiler_params=pltpu.CompilerParams(collective_id=0, has_side_effects=True, vmem_limit_bytes=50 * 2**20),
        )(mat_rows, tele_rows.T, dang_rows.reshape(-1, 128), damping, start_rows.T)
        return out.T

    return jax.shard_map(local_sweeps, mesh=mesh, in_specs=(spec_rows, spec_rows, spec_vec, P(None), spec_rows), out_specs=spec_rows, check_vma=False)
```

```python
import functools

import jax
import jax.numpy as jnp
from jax import lax
from jax.experimental import pallas as pl
from jax.experimental.pallas import tpu as pltpu
from jax.sharding import PartitionSpec as P

MESH = pl.DeviceIdType.MESH
TILE = 256
WIDE = 512
RING = 6
CROSS_AT = 11
LATER = {12: ((2, 0), (2, 1)), 13: ((2, 2), (2, 3)), 14: ((3, 0), (3, 1)), 15: ((3, 2),)}
OWN, SIB, CROSS, DIAG = range(4)


def _kernel(sweeps, seeds, nodes, mat_hbm, tele_ref, dang_ref, damp_ref, init_ref, out_ref,
            mat_t, stage, ranks, local_sum, mass,
            stage_sem, send_sem, recv_sem, msend_sem, mrecv_sem):
    part_rows = seeds // 2
    wides = nodes // WIDE
    tiles = nodes // TILE
    batch = lax.axis_index("batch")
    row = lax.axis_index("row")
    chip, core = row // 2, row % 2
    sib, cross, diag = chip * 2 + 1 - core, (1 - chip) * 2 + core, (1 - chip) * 2 + 1 - core
    blocks = (row, sib, cross, diag)

    def own_copy(par, ph, target):
        return pltpu.make_async_remote_copy(
            src_ref=ranks.at[par, OWN, ph], dst_ref=ranks.at[par, target, ph],
            send_sem=send_sem.at[par, ph], recv_sem=recv_sem.at[par, ph, target - 1],
            device_id=(batch, blocks[target]), device_id_type=MESH)

    def fwd_copy(par, ph):
        return pltpu.make_async_remote_copy(
            src_ref=ranks.at[par, CROSS, ph], dst_ref=ranks.at[par, DIAG, ph],
            send_sem=send_sem.at[par, ph], recv_sem=recv_sem.at[par, ph, DIAG - 1],
            device_id=(batch, sib), device_id_type=MESH)

    def mass_copy(par, ph, target):
        return pltpu.make_async_remote_copy(
            src_ref=mass.at[par, ph, OWN], dst_ref=mass.at[par, ph, target],
            send_sem=msend_sem.at[par, ph], recv_sem=mrecv_sem.at[par, ph],
            device_id=(batch, blocks[target]), device_id_type=MESH)

    def mass_all(par, ph):
        return pltpu.make_async_remote_copy(
            src_ref=mass.at[par, ph, 1:4], dst_ref=mass.at[par, ph, 1:4],
            send_sem=msend_sem.at[par, ph], recv_sem=mrecv_sem.at[par, ph],
            device_id=(batch, sib), device_id_type=MESH)

    def send(par, ph):
        own_copy(par, ph, CROSS).start()
        own_copy(par, ph, SIB).start()

    def mass_part(val, n, width):
        part = jnp.zeros((val.shape[0], 128), jnp.float32)
        for i in range(width // 128):
            r = n * (width // 128) + i
            part = part + val[:, i * 128:(i + 1) * 128] * dang_ref[r:r + 1, :].astype(jnp.float32)
        return part

    def send_mass(par, ph, part):
        mass[par, ph, OWN, 0:1, 0:part_rows] = jnp.sum(part.T, axis=0, keepdims=True)
        for target in (CROSS, DIAG, SIB):
            mass_copy(par, ph, target).start()

    def get_mass(par, ph):
        mass_all(par, ph).wait_recv()
        line = [mass[par, ph, s, 0:1, 0:part_rows] for s in range(4)]
        total = (line[OWN] + line[SIB]) + (line[CROSS] + line[DIAG])
        return jnp.broadcast_to(total, (128, part_rows)).T

    def stage_copy(i):
        s, n = i // wides, i % wides
        block = ((chip + s // 2) % 2) * 2 + (core + s % 2) % 2
        return pltpu.make_async_copy(
            mat_hbm.at[pl.ds(pl.multiple_of(n * WIDE, WIDE), WIDE), pl.ds(pl.multiple_of(block * nodes, nodes), nodes)],
            stage.at[i % RING], stage_sem.at[i % RING])

    for i in range(RING):
        stage_copy(i).start()

    mass[:, :, OWN] = jnp.zeros_like(mass[:, :, OWN])
    barrier = pltpu.get_barrier_semaphore()
    for peer in (sib, cross, diag):
        pl.semaphore_signal(barrier, inc=1, device_id=(batch, peer), device_id_type=MESH)
    pl.semaphore_wait(barrier, 3)

    for ph in range(2):
        rows = slice(ph * part_rows, (ph + 1) * part_rows)
        part = jnp.zeros((part_rows, 128), jnp.float32)
        for n in range(wides):
            val = init_ref[rows, n * WIDE:(n + 1) * WIDE]
            ranks[0, OWN, ph, :, n * WIDE:(n + 1) * WIDE] = val.astype(jnp.bfloat16)
            part = part + mass_part(val, n, WIDE)
        send(0, ph)
        send_mass(0, ph, part)

    def cols_of(n):
        return slice(n * WIDE, (n + 1) * WIDE)

    def lhs(par, s, ph):
        val = ranks[par, s, ph]
        return jnp.concatenate([val] * 4, axis=0)

    def dot(left, s, n):
        return jnp.dot(left, mat_t[s, n], preferred_element_type=jnp.float32)

    def local_pass(par):
        left = jnp.concatenate([ranks[par, OWN, 0], ranks[par, OWN, 1]] * 2, axis=0)
        for n in range(wides):
            local_sum[:, n * WIDE:(n + 1) * WIDE] = dot(left, OWN, n)[:seeds]
        for ph in range(2):
            own_copy(par, ph, SIB).wait_recv()
        left = jnp.concatenate([ranks[par, SIB, 0], ranks[par, SIB, 1]] * 2, axis=0)
        for n in range(wides):
            cols = slice(n * WIDE, (n + 1) * WIDE)
            local_sum[:, cols] = local_sum[:, cols] + dot(left, SIB, n)[:seeds]

    def remote_pass(par, ph, t, store):
        rows = slice(ph * part_rows, (ph + 1) * part_rows)
        own_copy(par, ph, CROSS).wait_recv()
        fwd_copy(par, ph).start()
        left = lhs(par, CROSS, ph)
        for n in range(wides):
            cols = slice(n * WIDE, (n + 1) * WIDE)
            local_sum[rows, cols] = local_sum[rows, cols] + dot(left, CROSS, n)[:part_rows]
        fwd_copy(par, ph).wait_recv()
        msum = get_mass(par, ph)
        factor = damp_ref[t]
        add = (factor * (1.0 / (4 * nodes))) * msum
        add = jnp.concatenate([add] * (WIDE // 128), axis=1)
        left = lhs(par, DIAG, ph)
        for n in range(wides):
            cols = slice(n * WIDE, (n + 1) * WIDE)
            total = local_sum[rows, cols] + dot(left, DIAG, n)[:part_rows]
            store(n, factor * total + (1.0 - factor) * tele_ref[rows, cols] + add)

    def done(par, ph):
        pltpu.make_async_remote_copy(
            src_ref=ranks.at[par, 0:3, ph], dst_ref=ranks.at[par, 0:3, ph],
            send_sem=send_sem.at[par, ph], recv_sem=recv_sem.at[par, ph, 0],
            device_id=(batch, sib), device_id_type=MESH).wait_send()
        mass_all(par, ph).wait_send()

    def load_piece(i):
        stage_copy(i).wait()
        for k in range(tiles):
            for u in range(WIDE // TILE):
                mat_t[i // wides, i % wides, k * TILE:(k + 1) * TILE, u * TILE:(u + 1) * TILE] = (
                    stage[i % RING, u * TILE:(u + 1) * TILE, k * TILE:(k + 1) * TILE].T)

        if i + RING < 4 * wides:
            stage_copy(i + RING).start()

    def both(par, s):
        return jnp.concatenate([ranks[par, s, 0], ranks[par, s, 1]] * 2, axis=0)

    def first_dot(s, n):
        prod = dot(both(0, s), s, n)[:seeds]
        local_sum[:, cols_of(n)] = prod if s == OWN else local_sum[:, cols_of(n)] + prod

    for i in range(4 * wides):
        if i == wides + 1:
            for ph in range(2):
                own_copy(0, ph, SIB).wait_recv()
        if i == CROSS_AT:
            for ph in range(2):
                own_copy(0, ph, CROSS).wait_recv()
                fwd_copy(0, ph).start()
        load_piece(i)
        if 1 <= i <= 2 * wides:
            first_dot((i - 1) // wides, (i - 1) % wides)
        if i == 4 * wides - 2:
            for ph in range(2):
                fwd_copy(0, ph).wait_recv()
        for s, n in LATER.get(i, ()):
            first_dot(s, n)
    first_parts = []
    sums = [get_mass(0, ph) for ph in range(2)]
    add = (damp_ref[0] * (1.0 / (4 * nodes))) * jnp.concatenate(sums, axis=0)
    add = jnp.concatenate([add] * (WIDE // 128), axis=1)
    for n in range(wides):
        total = local_sum[:, cols_of(n)]
        if n == wides - 1:
            total = total + dot(both(0, DIAG), DIAG, n)[:seeds]
        val = damp_ref[0] * total + (1.0 - damp_ref[0]) * tele_ref[:, cols_of(n)] + add
        for ph in range(2):
            ranks[1, OWN, ph, :, cols_of(n)] = val[ph * part_rows:(ph + 1) * part_rows].astype(jnp.bfloat16)
        first_parts.append(mass_part(val, n, WIDE))
    first_part = functools.reduce(jnp.add, first_parts)
    for ph in range(2):
        done(0, ph)
    for ph in range(2):
        send(1, ph)
        send_mass(1, ph, first_part[ph * part_rows:(ph + 1) * part_rows])

    def sweep(t, carry):
        par = lax.rem(t, 2)
        nxt = 1 - par
        local_pass(par)
        for ph in range(2):
            parts = []

            def store(n, val, ph=ph, parts=parts):
                ranks[nxt, OWN, ph, :, n * WIDE:(n + 1) * WIDE] = val.astype(jnp.bfloat16)
                parts.append(mass_part(val, n, WIDE))

            remote_pass(par, ph, t, store)
            done(par, ph)
            send(nxt, ph)
            send_mass(nxt, ph, functools.reduce(jnp.add, parts))
        return carry

    lax.fori_loop(1, sweeps - 1, sweep, 0)
    last = sweeps - 1
    par = last % 2
    local_pass(par)
    for ph in range(2):
        def store(n, val, ph=ph):
            out_ref[ph * part_rows:(ph + 1) * part_rows, n * WIDE:(n + 1) * WIDE] = val

        remote_pass(par, ph, last, store)
        done(par, ph)


def solution(mesh):
    spec_rows = P(("batch", "row"), None)
    spec_vec = P(("batch", "row"))

    def local_sweeps(mat_rows, tele_rows, dang_rows, damping, start_rows):
        nodes, seeds = start_rows.shape
        sweeps = damping.shape[0]
        hbm = pl.BlockSpec(memory_space=pl.ANY)
        vmem = pl.BlockSpec(memory_space=pltpu.VMEM)
        dma = pltpu.SemaphoreType.DMA
        out = pl.pallas_call(
            functools.partial(_kernel, sweeps, seeds, nodes),
            out_shape=jax.ShapeDtypeStruct((seeds, nodes), jnp.float32),
            in_specs=[hbm, vmem, vmem, pl.BlockSpec(memory_space=pltpu.SMEM), vmem],
            out_specs=vmem,
            scratch_shapes=[
                pltpu.VMEM((4, nodes // WIDE, nodes, WIDE), jnp.bfloat16),
                pltpu.VMEM((RING, WIDE, nodes), jnp.bfloat16),
                pltpu.VMEM((2, 4, 2, seeds // 2, nodes), jnp.bfloat16),
                pltpu.VMEM((seeds, nodes), jnp.float32),
                pltpu.VMEM((2, 2, 4, 8, 128), jnp.float32),
                dma((RING,)), dma((2, 2)), dma((2, 2, 3)), dma((2, 2)), dma((2, 2)),
            ],
            compiler_params=pltpu.CompilerParams(collective_id=0, has_side_effects=True, vmem_limit_bytes=50 * 2**20),
        )(mat_rows, tele_rows.T, dang_rows.reshape(-1, 128), damping, start_rows.T)
        return out.T

    return jax.shard_map(local_sweeps, mesh=mesh, in_specs=(spec_rows, spec_rows, spec_vec, P(None), spec_rows), out_specs=spec_rows, check_vma=False)
```
